256 devices in a mesh: seq: 32 (over z, x_lo, core), head: 8 (over y, x_hi).
Axes of the slice: x: 4 (x_hi: 2, x_lo: 2; x = x_hi * 2 + x_lo), y: 4, z: 8, core: 2. Of those that a mesh axis runs over, the one named last changes fastest.
Arguments:
- queries: bfloat16 [12288, 8192], P('seq', 'head'), may hold values from -6 to 6
- keys: bfloat16 [12288, 1024], P('seq', 'head'), may hold values from -6 to 6
- values: bfloat16 [12288, 1024], P('seq', 'head'), may hold values from -6 to 6
- windows: int32 [8], P('head'), may hold values from 256 to 4096, as said below
- out_weight: bfloat16 [8192, 8192], P('head', 'seq'), may hold values from -0.0625 to 0.0625
Outputs:
- projected: bfloat16 [12288, 8192], P('seq', 'head')
The draws below stay inside these ranges and needn't reach their ends.
Inputs may be any that keep to these rules, and one draw needn't show every extreme that they name: `windows`: every window is a multiple of 128; in every draw some group has exactly 4096, and where there are three groups or more another has exactly 256.
All inputs are finite; a program needn't handle non-finite values.
Results may differ from the reference program's by a relative error of at most 0.014.
Values may be sent and summed in bfloat16 or wider, within the bound.
A program may use at most 128 MiB of HBM per device.

```python
import math
import jax
import jax.numpy as jnp
from jax import lax

D = 8192
DH = 128
QPG = 8
TOK_DEV = 384
WMAX = 4096
WMIN = 256
WSTEP = 128
KVH = 8
HEADS = 64
TOKENS = 12288


def draw_queries(key, part):
    first_key_index = jax.random.fold_in(key, 1)
    shape = (TOKENS, KVH, QPG, DH)
    base = jax.random.truncated_normal(first_key_index, -4.0, 4.0, shape, jnp.float32)
    return base.reshape(TOKENS, KVH * QPG * DH).astype(jnp.bfloat16)


def draw_keys(key, part):
    first_key_index = jax.random.fold_in(key, 2)
    shape = (TOKENS, KVH, DH)
    base = jax.random.truncated_normal(first_key_index, -4.0, 4.0, shape, jnp.float32)
    return base.reshape(TOKENS, KVH * DH).astype(jnp.bfloat16)


def draw_windows(key, part):
    counts = jax.random.randint(jax.random.fold_in(key, 5), (KVH,), WMIN // WSTEP, WMAX // WSTEP + 1, jnp.int32)
    spans = counts * WSTEP
    order = jax.random.permutation(jax.random.fold_in(key, 6), KVH)
    spans = spans.at[order[0]].set(WMAX)
    if KVH > 2:
        spans = spans.at[order[1]].set(WMIN)
    return spans.astype(jnp.int32)


def block_levels(own_key, shape, cuts, least, top_value):
    loudness, own = 1.0, jax.random.fold_in(own_key, 6)
    for dim, shards_of in cuts:
        heights = jnp.exp(jax.random.uniform(jax.random.fold_in(own, dim), (shards_of,), jnp.float32, least / len(cuts), top_value / len(cuts)))
        loudness = loudness * jnp.repeat(heights, shape[dim] // shards_of).reshape([-1 if axis == dim else 1 for axis in range(len(shape))])
    return loudness


def noise(key, shape, scale, most, split=(), held_as=jnp.bfloat16):
    result = jax.random.normal(key, shape, jnp.float32) * scale
    if len(split) > 0:
        result = block_levels(key, shape, split, -0.22, 0.18) * result
    return jnp.clip(result, min=-most, max=most).astype(held_as)


def setup_inputs(seed: int = 0) -> dict:
    splits = jax.random.split(jax.random.key(seed), 6)
    return {
        "queries": draw_queries(jax.random.fold_in(splits[5], 71), 0),
        "keys": draw_keys(jax.random.fold_in(splits[5], 71), 0),
        "values": noise(splits[2], (TOKENS, KVH * DH), 1.0, 6.0, ((0, 32), (1, 8))),
        "windows": draw_windows(jax.random.fold_in(splits[5], 71), 0),
        "out_weight": noise(splits[4], (HEADS * DH, D), (HEADS * DH) ** -0.5, 0.0625, ((0, 8), (1, 32))),
    }


def reference(queries, keys, values, windows, out_weight):
    blocks_total = TOKENS // TOK_DEV
    halo_len = (WMAX + TOK_DEV - 2) // TOK_DEV * TOK_DEV
    score_scale = 1.0 / math.sqrt(DH)
    key_pad = jnp.concatenate([jnp.zeros((halo_len, KVH * DH), keys.dtype), keys], 0)
    value_pad = jnp.concatenate([jnp.zeros((halo_len, KVH * DH), values.dtype), values], 0)
    spans = windows.astype(jnp.int32)

    def single_block_attend(block_index):
        first = (block_index * TOK_DEV).astype(jnp.int32)
        query_block = lax.dynamic_slice_in_dim(queries, first, TOK_DEV, 0).reshape(TOK_DEV, KVH, QPG, DH).astype(jnp.float32)
        key_block = lax.dynamic_slice_in_dim(key_pad, first, halo_len + TOK_DEV, 0).reshape(halo_len + TOK_DEV, KVH, DH).astype(jnp.float32)
        value_block = lax.dynamic_slice_in_dim(value_pad, first, halo_len + TOK_DEV, 0).reshape(halo_len + TOK_DEV, KVH, DH).astype(jnp.float32)
        scores = jnp.einsum('igpd,jgd->gpij', query_block, key_block) * score_scale
        query_pos = first + jnp.arange(TOK_DEV, dtype=jnp.int32)
        key_pos = first - halo_len + jnp.arange(halo_len + TOK_DEV, dtype=jnp.int32)
        allowed = (key_pos[None, None, :] <= query_pos[None, :, None]) & (key_pos[None, None, :] > query_pos[None, :, None] - spans[:, None, None]) & (key_pos[None, None, :] >= 0)
        allowed = allowed[:, None]
        masked = jnp.where(allowed, scores, -1e+30)
        peak_score_running = lax.optimization_barrier(jnp.max(masked, axis=-1, keepdims=True))
        weights = jnp.where(allowed, jnp.exp(scores - peak_score_running), 0.0)
        total = lax.optimization_barrier(jnp.sum(weights, axis=-1))
        rounded = lax.optimization_barrier(weights.astype(jnp.bfloat16)).astype(jnp.float32)
        mixed = jnp.einsum('gpij,jgd->igpd', rounded, value_block)
        mixed = mixed / jnp.transpose(total, (2, 0, 1))[..., None]
        return mixed.astype(jnp.bfloat16).reshape(TOK_DEV, KVH * QPG * DH)
    attended = lax.map(single_block_attend, jnp.arange(blocks_total, dtype=jnp.int32))
    attended = attended.reshape(TOKENS, KVH * QPG * DH)
    return jnp.dot(attended, out_weight, preferred_element_type=jnp.float32).astype(jnp.bfloat16)
```

```python
import math

import jax
import jax.numpy as jnp
from jax import lax
from jax.experimental import pallas as pl
from jax.experimental.pallas import tpu as pltpu
from jax.sharding import PartitionSpec as P

MESH = pl.DeviceIdType.MESH
DH = 128
QPG = 8
T = 384
NZ = 8
NEG = -1e30
ROWS = 2 * T
PAIRS = QPG // 2
VR = DH + 16
C = 256
F32 = jnp.float32
BF16 = jnp.bfloat16
NT = (((1,), (1,)), ((), ()))
NN = (((1,), (0,)), ((), ()))


def dot(a, b, dims=NN):
    return lax.dot_general(a, b, dims, preferred_element_type=F32)


def kernel(q_ref, k_ref, v_ref, win_ref, w_ref, out_ref,
           qs, k_all, vt_all, w_all, a_all, s_ref, m_ref, acc_ref, fb_ref, bias0, kb, vb, tb,
           tx, rx, keep, xtx, xrx, fin,
           lsem, zs, zr, xs, xr, ss, sr, fs, fr, wds, wdr, wus, wur,
           axs, axr, ass, asr, afs, afr, ys, yr, hs, hr, os, orr):
    seq = lax.axis_index("seq")
    head = lax.axis_index("head")
    z = seq // 4
    q = seq % 4
    y = head // 2
    xh = head % 2
    q1 = q + 1 - 2 * (q % 2)
    q2 = (q + 2) % 4
    q3 = q1 + 2 - 4 * (q1 // 2)
    zup = (((z + 1) % NZ) * 4 + q, head)
    zdn = (((z + NZ - 1) % NZ) * 4 + q, head)
    sib = (z * 4 + q1, head)
    xlo = (z * 4 + q2, head)
    dia = (z * 4 + q3, head)
    yup = (seq, ((y + 1) % 4) * 2 + xh)
    ydn = (seq, ((y + 3) % 4) * 2 + xh)
    xhi = (seq, y * 2 + 1 - xh)

    def rc(src, dst, ssem, rsem, dev):
        return pltpu.make_async_remote_copy(
            src_ref=src, dst_ref=dst, send_sem=ssem, recv_sem=rsem, device_id=dev, device_id_type=MESH)

    lk = pltpu.make_async_copy(k_ref, k_all.at[3], lsem.at[0])
    lw = pltpu.make_async_copy(w_ref, w_all.at[0], lsem.at[1])
    lk.start()
    lw.start()
    barrier = pltpu.get_barrier_semaphore()
    for dev in (zup, zdn, sib, xlo, dia, yup, ydn, xhi):
        pl.semaphore_signal(barrier, inc=1, device_id=dev, device_id_type=MESH)
    for slot in range(19):
        vt_all[slot, DH:VR, :] = jnp.ones((VR - DH, T), BF16)
    vt_all[3, 0:DH, :] = v_ref[...].astype(F32).T.astype(BF16)
    lk.wait()
    lw.wait()
    pl.semaphore_wait(barrier, 8)

    def kv(src_slot, dst_slot, ssem, rsem, n, dev):
        return (rc(k_all.at[src_slot], k_all.at[dst_slot], ssem.at[n, 0], rsem.at[n, 0], dev),
                rc(vt_all.at[src_slot, pl.ds(0, DH)], vt_all.at[dst_slot, pl.ds(0, DH)],
                   ssem.at[n, 1], rsem.at[n, 1], dev))

    def kv_z(dz):
        return kv(3 + 4 * dz, 7 + 4 * dz, zs, zr, dz, zup)

    def kv_x(dz):
        return kv(3 + 4 * dz, 3 + 4 * dz + q2 - q, xs, xr, dz, xlo)

    def kv_s(dz):
        return kv(3 + 4 * dz, 3 + 4 * dz + q1 - q, ss, sr, dz, sib)

    def kv_f(dz):
        return kv(3 + 4 * dz + q - q2, 3 + 4 * dz + q1 - q2, fs, fr, dz, sib)

    def w_dn(n):
        return rc(w_all.at[n], w_all.at[n + 1], wds.at[n], wdr.at[n], zdn)

    def w_up(n):
        return rc(w_all.at[(NZ - n) % NZ], w_all.at[NZ - 1 - n], wus.at[n], wur.at[n], zup)

    def start(*copies):
        for c in copies:
            c.start()

    def got(*copies):
        for c in copies:
            c.wait_recv()

    start(*kv_z(0), *kv_x(0), *kv_s(0))
    start(w_dn(0))

    for p in range(QPG):
        qs[p // 2, (p % 2) * T:(p % 2 + 1) * T, :] = (
            q_ref[:, p * DH:(p + 1) * DH].astype(F32) * (math.log2(math.e) / math.sqrt(DH))).astype(BF16)
    wn = win_ref[0] // 128
    col = lax.broadcasted_iota(jnp.int32, (1, ROWS), 1)
    ctile = sum(jnp.where(col >= 128 * n, 1, 0) for n in range(1, 6))
    iq = ctile - 3 * jnp.where(ctile >= 3, 1, 0)
    for d in range(1, 12):
        for jk in range(3):
            inside = (3 * d - jk + iq < wn) & (seq - d >= 0)
            fb_ref[d * 3 + jk] = jnp.where(inside, 0.0, NEG)
    kj = lax.broadcasted_iota(jnp.int32, (T, T), 0)
    qi = lax.broadcasted_iota(jnp.int32, (T, T), 1)
    kt = jnp.where(kj >= 128, 1, 0) + jnp.where(kj >= 256, 1, 0)
    qt = jnp.where(qi >= 128, 1, 0) + jnp.where(qi >= 256, 1, 0)
    bias0[...] = jnp.where((kj <= qi) & (qt - kt < wn), 0.0, NEG)

    def group(dlist, first, last):
        def pair_body(pr, carry):
            qp = qs[pr]
            mx = None
            for b, d in enumerate(dlist):
                s = dot(k_all[d + 3], qp, NT)
                if d == 0:
                    s = s + jnp.concatenate([bias0[...], bias0[...]], axis=1)
                s_ref[b] = s
                for jk in range(3):
                    t8 = jnp.max(s[jk * 128:(jk + 1) * 128].reshape(16, 8, ROWS), axis=0)
                    if d > 0:
                        t8 = t8 + fb_ref[d * 3 + jk]
                    mx = t8 if mx is None else jnp.maximum(mx, t8)
            edge = []
            if last:
                for c in range(6):
                    sb = dot(kb[c % 3], qp[c * 128:(c + 1) * 128], NT) + tb[c % 3]
                    edge.append(sb)
                e8 = [jnp.max(sb.reshape(16, 8, 128), axis=0) for sb in edge]
                mx = jnp.maximum(mx, jnp.concatenate(e8, axis=1))
            m_new = jnp.max(mx, axis=0, keepdims=True)
            if not first:
                m_old = m_ref[pr]
                m_new = jnp.maximum(m_old, m_new)
                alpha = jnp.exp2(m_old - m_new)
            pv = None
            for b, d in enumerate(dlist):
                tiles = []
                for jk in range(3):
                    shift = m_new - fb_ref[d * 3 + jk] if d > 0 else m_new
                    tiles.append(jnp.exp2(s_ref[b, jk * 128:(jk + 1) * 128, :] - shift).astype(BF16))
                part = dot(vt_all[d + 3], jnp.concatenate(tiles, axis=0))
                pv = part if pv is None else pv + part
            if last:
                ep = []
                for c in range(6):
                    pe = jnp.exp2(edge[c] - m_new[:, c * 128:(c + 1) * 128]).astype(BF16)
                    ep.append(dot(vb[c % 3], pe))
                pv = pv + jnp.concatenate(ep, axis=1)
            if not first:
                pv = acc_ref[pr] * alpha + pv
            if last:
                o = pv[0:DH] / pv[DH:DH + 1]
                for h in range(2):
                    a_all[q, pr, :, h * DH:(h + 1) * DH] = o[:, h * T:(h + 1) * T].T.astype(BF16)
                start(a_x(pr), a_s(pr))
            else:
                acc_ref[pr] = pv
                m_ref[pr] = m_new
            return carry

        lax.fori_loop(0, PAIRS, pair_body, 0)

    def a_x(pr):
        return rc(a_all.at[q, pr], a_all.at[q, pr], axs.at[pr], axr.at[pr], xlo)

    def a_s(pr):
        return rc(a_all.at[q, pr], a_all.at[q, pr], ass.at[pr], asr.at[pr], sib)

    def a_f(pr):
        return rc(a_all.at[q2, pr], a_all.at[q2, pr], afs.at[pr], afr.at[pr], sib)

    group((0,), True, False)
    got(*kv_z(0))
    start(*kv_z(1), *kv_x(1), *kv_s(1))
    got(*kv_x(0))
    start(*kv_f(0))
    got(*kv_z(1))
    start(*kv_z(2), *kv_x(2), *kv_s(2))
    start(w_up(0))
    got(*kv_x(1))
    start(*kv_f(1))
    got(*kv_s(0), *kv_s(1), *kv_f(0), *kv_f(1))
    group((1, 2, 3), False, False)
    got(w_dn(0))
    start(w_dn(1))
    got(*kv_z(2))
    start(*kv_x(3), *kv_s(3))
    got(*kv_x(2))
    start(*kv_f(2))
    got(*kv_s(2), *kv_f(2))
    group((4, 5, 6, 7), False, False)
    got(*kv_x(3))
    start(*kv_f(3))
    got(*kv_s(3), *kv_f(3))
    got(w_dn(1))
    start(w_dn(2))
    got(w_up(0))
    start(w_up(1))
    ej = lax.broadcasted_iota(jnp.int32, (128, 128), 0)
    ei = lax.broadcasted_iota(jnp.int32, (128, 128), 1)
    for n in range(3):
        kn = jnp.zeros((128, DH), BF16)
        vn = jnp.zeros((VR, 128), BF16)
        for d in range(12):
            for jk in range(3):
                if 2 <= 3 * d + n - jk <= 32:
                    here = wn == 3 * d + n - jk
                    kn = jnp.where(here, k_all[d + 3, jk * 128:(jk + 1) * 128, :], kn)
                    vn = jnp.where(here, vt_all[d + 3, :, jk * 128:(jk + 1) * 128], vn)
        kb[n] = kn
        vb[n] = vn
        tb[n] = jnp.where((ej > ei) & (3 * seq + n - wn >= 0), 0.0, NEG)
    group((8, 9, 10, 11), False, True)

    for pr in range(PAIRS):
        got(a_x(pr))
        start(a_f(pr))
    got(w_dn(2))
    start(w_dn(3))
    got(w_up(1))
    start(w_up(2))
    for pr in range(PAIRS):
        got(a_s(pr), a_f(pr))
    got(w_dn(3), w_up(2))

    def ycopy(rb, way, n):
        return rc(tx.at[rb, way, n], rx.at[rb, way, n], ys.at[rb, way, n], yr.at[rb, way, n], yup if way == 0 else ydn)

    def hcopy(rb):
        return rc(xtx.at[rb], xrx.at[rb], hs.at[rb], hr.at[rb], xhi)

    def ocopy(rb, dev_q, slot):
        cols = pl.ds(pl.multiple_of(slot * C, C), C)
        return rc(fin.at[rb], out_ref.at[:, cols], os.at[rb], orr.at[slot], (z * 4 + dev_q, head))

    def project(rb, yd, half):
        r = (((y + yd) % 4) * 2 + half + NZ - z) % NZ
        total = None
        for pr in range(PAIRS):
            part = dot(a_all[rb, pr], w_all[r, pr * C:(pr + 1) * C, :])
            total = part if total is None else total + part
        return total

    def first_stage(rb):
        for way in range(2):
            tx[rb, way, 0] = project(rb, 2, way).astype(BF16)
            start(ycopy(rb, way, 0))
        for way in range(2):
            tx[rb, way, 1] = project(rb, 1 if way == 0 else 3, 1 - way).astype(BF16)
            start(ycopy(rb, way, 1))
        for way in range(2):
            keep[rb, way] = project(rb, 1 if way == 0 else 3, way)
        for half in range(2):
            keep[rb, 2 + half] = project(rb, 0, half)

    def second_stage(rb):
        for way in range(2):
            got(ycopy(rb, way, 0))
            tx[rb, way, 2] = (keep[rb, way] + rx[rb, way, 0].astype(F32)).astype(BF16)
            start(ycopy(rb, way, 2))

    def third_stage(rb):
        for n in (1, 2):
            for way in range(2):
                got(ycopy(rb, way, n))
        for half in range(2):
            keep[rb, 2 + half] = keep[rb, 2 + half] + (
                rx[rb, half, 2].astype(F32) + rx[rb, 1 - half, 1].astype(F32))
        xtx[rb] = keep[rb, 3 - xh].astype(BF16)
        start(hcopy(rb))

    def fourth_stage(rb):
        got(hcopy(rb))
        total = (keep[rb, 2 + xh] + xrx[rb].astype(F32)).astype(BF16)
        fin[rb] = total

        @pl.when(rb != q)
        def _():
            start(ocopy(rb, rb, q))

    def rb_loop(t, carry):
        for lag, (stage) in enumerate((first_stage, second_stage, third_stage, fourth_stage)):
            @pl.when((t >= lag) & (t < 4 + lag))
            def _():
                stage(t - lag)
        return carry

    lax.fori_loop(0, 7, rb_loop, 0)
    out_ref[:, pl.ds(pl.multiple_of(q * C, C), C)] = fin[q]

    for c in kv_z(0) + kv_z(1) + kv_z(2):
        c.wait_send()
    for dz in range(4):
        for c in kv_x(dz) + kv_s(dz) + kv_f(dz):
            c.wait_send()
    for n in range(4):
        w_dn(n).wait_send()
    for n in range(3):
        w_up(n).wait_send()
    for pr in range(PAIRS):
        for c in (a_x(pr), a_s(pr), a_f(pr)):
            c.wait_send()

    def finish(rb, carry):
        for way in range(2):
            for n in range(3):
                ycopy(rb, way, n).wait_send()
        hcopy(rb).wait_send()

        @pl.when(rb != q)
        def _():
            ocopy(rb, rb, q).wait_send()
            ocopy(rb, rb, rb).wait_recv()

        return carry

    lax.fori_loop(0, 4, finish, 0)


def body(queries, keys, values, windows, out_weight):
    dma = pltpu.SemaphoreType.DMA
    vm = pl.BlockSpec(memory_space=pltpu.VMEM)
    hbm = pl.BlockSpec(memory_space=pl.ANY)
    return pl.pallas_call(
        kernel,
        out_shape=jax.ShapeDtypeStruct((T, 4 * C), BF16),
        in_specs=[vm, hbm, vm, pl.BlockSpec(memory_space=pltpu.SMEM), hbm],
        out_specs=vm,
        scratch_shapes=[
            pltpu.VMEM((PAIRS, ROWS, DH), BF16),
            pltpu.VMEM((19, T, DH), BF16),
            pltpu.VMEM((19, VR, T), BF16),
            pltpu.VMEM((NZ, QPG * DH, C), BF16),
            pltpu.VMEM((4, PAIRS, T, C), BF16),
            pltpu.VMEM((4, T, ROWS), F32),
            pltpu.VMEM((PAIRS, 1, ROWS), F32),
            pltpu.VMEM((PAIRS, VR, ROWS), F32),
            pltpu.VMEM((36, 1, ROWS), F32),
            pltpu.VMEM((T, T), F32),
            pltpu.VMEM((3, 128, DH), BF16),
            pltpu.VMEM((3, VR, 128), BF16),
            pltpu.VMEM((3, 128, 128), F32),
            pltpu.VMEM((4, 2, 3, T, C), BF16),
            pltpu.VMEM((4, 2, 3, T, C), BF16),
            pltpu.VMEM((4, 4, T, C), F32),
            pltpu.VMEM((4, T, C), BF16),
            pltpu.VMEM((4, T, C), BF16),
            pltpu.VMEM((4, T, C), BF16),
            dma((2,)),
            dma((3, 2)), dma((3, 2)),
            dma((4, 2)), dma((4, 2)),
            dma((4, 2)), dma((4, 2)),
            dma((4, 2)), dma((4, 2)),
            dma((4,)), dma((4,)),
            dma((3,)), dma((3,)),
            dma((PAIRS,)), dma((PAIRS,)),
            dma((PAIRS,)), dma((PAIRS,)),
            dma((PAIRS,)), dma((PAIRS,)),
            dma((4, 2, 3)), dma((4, 2, 3)),
            dma((4,)), dma((4,)),
            dma((4,)), dma((4,)),
        ],
        compiler_params=pltpu.CompilerParams(
            collective_id=0, has_side_effects=True, vmem_limit_bytes=60 * 1024 * 1024),
        name="fused",
    )(queries, keys, values, windows, out_weight)


def solution(mesh):
    placed = (P("seq", "head"), P("seq", "head"), P("seq", "head"), P("head"), P("head", "seq"))
    return jax.shard_map(
        body, mesh=mesh, in_specs=placed, out_specs=P("seq", "head"), check_vma=False
    )
```

```python
import math

import jax
import jax.numpy as jnp
from jax import lax
from jax.experimental import pallas as pl
from jax.experimental.pallas import tpu as pltpu
from jax.sharding import PartitionSpec as P

MESH = pl.DeviceIdType.MESH
DH = 128
QPG = 8
T = 384
NZ = 8
H = T // 2
NEG = -1e30
ROWS = 2 * T
PAIRS = QPG // 2
VR = DH + 16
C = 256
F32 = jnp.float32
BF16 = jnp.bfloat16
NT = (((1,), (1,)), ((), ()))
NN = (((1,), (0,)), ((), ()))


def dot(a, b, dims=NN):
    return lax.dot_general(a, b, dims, preferred_element_type=F32)


def kernel(q_ref, k_ref, v_ref, win_ref, w_ref, out_ref,
           qs, k_all, vt_all, w_all, a_all, s_ref, m_ref, acc_ref, fb_ref, bias0, kb, vb, tb,
           tx, rx, keep, xtx, xrx, fin,
           lsem, zs, zr, xs, xr, ss, sr, fs, fr, wds, wdr, wus, wur,
           axs, axr, ass, asr, afs, afr, ys, yr, hs, hr, os, orr):
    seq = lax.axis_index("seq")
    head = lax.axis_index("head")
    z = seq // 4
    q = seq % 4
    y = head // 2
    xh = head % 2
    q1 = q + 1 - 2 * (q % 2)
    q2 = (q + 2) % 4
    q3 = q1 + 2 - 4 * (q1 // 2)
    zup = (((z + 1) % NZ) * 4 + q, head)
    zdn = (((z + NZ - 1) % NZ) * 4 + q, head)
    sib = (z * 4 + q1, head)
    xlo = (z * 4 + q2, head)
    dia = (z * 4 + q3, head)
    yup = (seq, ((y + 1) % 4) * 2 + xh)
    ydn = (seq, ((y + 3) % 4) * 2 + xh)
    xhi = (seq, y * 2 + 1 - xh)

    def rc(src, dst, ssem, rsem, dev):
        return pltpu.make_async_remote_copy(
            src_ref=src, dst_ref=dst, send_sem=ssem, recv_sem=rsem, device_id=dev, device_id_type=MESH)

    lk = pltpu.make_async_copy(k_ref, k_all.at[3], lsem.at[0])
    lw = pltpu.make_async_copy(w_ref, w_all.at[0], lsem.at[1])
    lk.start()
    lw.start()
    barrier = pltpu.get_barrier_semaphore()
    for dev in (zup, zdn, sib, xlo, dia, yup, ydn, xhi):
        pl.semaphore_signal(barrier, inc=1, device_id=dev, device_id_type=MESH)
    for slot in range(19):
        vt_all[slot, DH:VR, :] = jnp.ones((VR - DH, T), BF16)
    vt_all[3, 0:DH, :] = v_ref[...].astype(F32).T.astype(BF16)
    lk.wait()
    lw.wait()
    pl.semaphore_wait(barrier, 8)

    def kv(src_slot, dst_slot, ssem, rsem, n, i, dev):
        if i == 0:
            return rc(k_all.at[src_slot], k_all.at[dst_slot], ssem.at[n, 0], rsem.at[n, 0], dev)
        return rc(vt_all.at[src_slot, pl.ds(0, DH)], vt_all.at[dst_slot, pl.ds(0, DH)],
                  ssem.at[n, 1], rsem.at[n, 1], dev)

    def kv_z(dz, i):
        return kv(3 + 4 * dz, 7 + 4 * dz, zs, zr, dz, i, zup)

    def kv_x(dz, i):
        return kv(3 + 4 * dz, 3 + 4 * dz + q2 - q, xs, xr, dz, i, xlo)

    def kv_s(dz, i):
        return kv(3 + 4 * dz, 3 + 4 * dz + q1 - q, ss, sr, dz, i, sib)

    def kv_f(dz, i):
        return kv(3 + 4 * dz + q - q2, 3 + 4 * dz + q1 - q2, fs, fr, dz, i, sib)

    def only(dz, near, far, act):
        if dz in (1, 2):
            act()
        else:
            pl.when(near if dz == 0 else far)(act)

    low, even = q < 2, q % 2 == 0
    high, odd = q >= 2, q % 2 == 1

    def send_z(dz, i):
        kv_z(dz, i).start()

    def send_xs(dz, i):
        only(dz, low, high, lambda: kv_x(dz, i).start())
        only(dz, even, odd, lambda: kv_s(dz, i).start())

    def pass_f(dz, i):
        def act():
            kv_x(dz, i).wait_recv()
            kv_f(dz, i).start()
        only(dz, high, low, act)

    def got_sf(dz):
        for i in range(2):
            only(dz, odd, even, lambda: kv_s(dz, i).wait_recv())
            only(dz, high, low, lambda: kv_f(dz, i).wait_recv())

    def w_dn(n, hf):
        rows = pl.ds(hf * 256, 256)
        return rc(w_all.at[n, rows], w_all.at[n + 1, rows], wds.at[n, hf], wdr.at[n, hf], zdn)

    def w_up(n, hf):
        rows = pl.ds(hf * 256, 256)
        return rc(w_all.at[(NZ - n) % NZ, rows], w_all.at[NZ - 1 - n, rows], wus.at[n, hf], wur.at[n, hf], zup)

    def start(*copies):
        for c in copies:
            c.start()

    def got(*copies):
        for c in copies:
            c.wait_recv()

    def pass_dn(n, hf):
        got(w_dn(n, hf))
        start(w_dn(n + 1, hf))

    def pass_up(n, hf):
        got(w_up(n, hf))
        start(w_up(n + 1, hf))

    for i in range(2):
        send_z(0, i)
        send_xs(0, i)
    start(*[w_dn(0, hf) for hf in range(4)], w_up(0, 0))

    for p in range(QPG):
        qs[p // 2, (p % 2) * T:(p % 2 + 1) * T, :] = (
            q_ref[:, p * DH:(p + 1) * DH].astype(F32) * (math.log2(math.e) / math.sqrt(DH))).astype(BF16)
    wn = win_ref[0] // 128
    col = lax.broadcasted_iota(jnp.int32, (1, ROWS), 1)
    ctile = sum(jnp.where(col >= 128 * n, 1, 0) for n in range(1, 6))
    iq = ctile - 3 * jnp.where(ctile >= 3, 1, 0)
    for d in range(1, 12):
        for jk in range(3):
            inside = (3 * d - jk + iq < wn) & (seq - d >= 0)
            fb_ref[d * 3 + jk] = jnp.where(inside, 0.0, NEG)
    kj = lax.broadcasted_iota(jnp.int32, (T, T), 0)
    qi = lax.broadcasted_iota(jnp.int32, (T, T), 1)
    kt = jnp.where(kj >= 128, 1, 0) + jnp.where(kj >= 256, 1, 0)
    qt = jnp.where(qi >= 128, 1, 0) + jnp.where(qi >= 256, 1, 0)
    bias0[...] = jnp.where((kj <= qi) & (qt - kt < wn), 0.0, NEG)

    def group(dlist, first, last, service=()):
        def pair_body(pr, carry):
            for at, act in service:
                pl.when(pr == at)(act)
            qp = qs[pr]
            mx = None
            for b, d in enumerate(dlist):
                s = dot(k_all[d + 3], qp, NT)
                if d == 0:
                    s = s + jnp.concatenate([bias0[...], bias0[...]], axis=1)
                s_ref[b] = s
                for jk in range(3):
                    t8 = jnp.max(s[jk * 128:(jk + 1) * 128].reshape(16, 8, ROWS), axis=0)
                    if d > 0:
                        t8 = t8 + fb_ref[d * 3 + jk]
                    mx = t8 if mx is None else jnp.maximum(mx, t8)
            edge = []
            if last:
                for c in range(6):
                    sb = dot(kb[c % 3], qp[c * 128:(c + 1) * 128], NT) + tb[c % 3]
                    edge.append(sb)
                e8 = [jnp.max(sb.reshape(16, 8, 128), axis=0) for sb in edge]
                mx = jnp.maximum(mx, jnp.concatenate(e8, axis=1))
            m_new = jnp.max(mx, axis=0, keepdims=True)
            if not first:
                m_old = m_ref[pr]
                m_new = jnp.maximum(m_old, m_new)
                alpha = jnp.exp2(m_old - m_new)
            pv = None
            for b, d in enumerate(dlist):
                tiles = []
                for jk in range(3):
                    shift = m_new - fb_ref[d * 3 + jk] if d > 0 else m_new
                    tiles.append(jnp.exp2(s_ref[b, jk * 128:(jk + 1) * 128, :] - shift).astype(BF16))
                part = dot(vt_all[d + 3], jnp.concatenate(tiles, axis=0))
                pv = part if pv is None else pv + part
            if last:
                ep = []
                for c in range(6):
                    pe = jnp.exp2(edge[c] - m_new[:, c * 128:(c + 1) * 128]).astype(BF16)
                    ep.append(dot(vb[c % 3], pe))
                pv = pv + jnp.concatenate(ep, axis=1)
            if not first:
                pv = acc_ref[pr] * alpha + pv
            if last:
                o = pv[0:DH] / pv[DH:DH + 1]
                for h in range(2):
                    a_all[q, pr, :, h * DH:(h + 1) * DH] = o[:, h * T:(h + 1) * T].T.astype(BF16)
                start(a_x(pr), a_s(pr))
            else:
                acc_ref[pr] = pv
                m_ref[pr] = m_new
            return carry

        lax.fori_loop(0, PAIRS, pair_body, 0)

    def a_x(pr):
        return rc(a_all.at[q, pr], a_all.at[q, pr], axs.at[pr], axr.at[pr], xlo)

    def a_s(pr):
        return rc(a_all.at[q, pr], a_all.at[q, pr], ass.at[pr], asr.at[pr], sib)

    def a_f(pr):
        return rc(a_all.at[q2, pr], a_all.at[q2, pr], afs.at[pr], afr.at[pr], sib)

    group((0,), True, False)
    for i in range(2):
        got(kv_z(0, i))
        send_z(1, i)
        send_xs(1, i)
    start(w_up(0, 1))
    for i in range(2):
        pass_f(0, i)
    for i in range(2):
        got(kv_z(1, i))
        send_z(2, i)
        send_xs(2, i)
    start(w_up(0, 2), w_up(0, 3))
    pass_dn(0, 0)
    pass_dn(0, 1)
    for i in range(2):
        pass_f(1, i)
    pass_dn(0, 2)
    got_sf(0)
    got_sf(1)

    def in_first():
        for i in range(2):
            got(kv_z(2, i))
            send_xs(3, i)
        pass_dn(0, 3)
        pass_up(0, 0)

    group((1, 2, 3), False, False, ((2, in_first),))
    for i in range(2):
        pass_f(2, i)
    pass_dn(1, 0)
    got_sf(2)

    def in_second():
        pass_dn(1, 1)
        pass_up(0, 1)
        for i in range(2):
            pass_f(3, i)

    def late_second():
        pass_dn(1, 2)
        pass_up(0, 2)

    group((4, 5, 6, 7), False, False, ((1, in_second), (3, late_second)))
    got_sf(3)
    pass_dn(1, 3)
    pass_up(0, 3)

    def in_third():
        pass_dn(2, 0)
        pass_up(1, 0)

    def late_third():
        pass_dn(2, 1)
        pass_up(1, 1)

    ej = lax.broadcasted_iota(jnp.int32, (128, 128), 0)
    ei = lax.broadcasted_iota(jnp.int32, (128, 128), 1)
    for n in range(3):
        kn = jnp.zeros((128, DH), BF16)
        vn = jnp.zeros((VR, 128), BF16)
        for d in range(12):
            for jk in range(3):
                if 2 <= 3 * d + n - jk <= 32:
                    here = wn == 3 * d + n - jk
                    kn = jnp.where(here, k_all[d + 3, jk * 128:(jk + 1) * 128, :], kn)
                    vn = jnp.where(here, vt_all[d + 3, :, jk * 128:(jk + 1) * 128], vn)
        kb[n] = kn
        vb[n] = vn
        tb[n] = jnp.where((ej > ei) & (3 * seq + n - wn >= 0), 0.0, NEG)
    group((8, 9, 10, 11), False, True, ((1, in_third), (3, late_third)))
    for hf in (2, 3):
        pass_dn(2, hf)
        pass_up(1, hf)
    for pr in range(PAIRS):
        got(a_x(pr))
        start(a_f(pr))
    for pr in range(PAIRS):
        got(a_s(pr), a_f(pr))
    for hf in range(4):
        got(w_dn(3, hf), w_up(2, hf))

    def ycopy(rb, way, n):
        return rc(tx.at[rb, way, n], rx.at[rb, way, n], ys.at[rb, way, n], yr.at[rb, way, n], yup if way == 0 else ydn)

    def hcopy(rb):
        return rc(xtx.at[rb], xrx.at[rb], hs.at[rb], hr.at[rb], xhi)

    def ocopy(rb, dev_q, slot):
        rows, cols = span(rb), pl.ds(pl.multiple_of(slot * C, C), C)
        return rc(fin.at[rb], out_ref.at[rows, cols], os.at[rb], orr.at[slot, rb % 2], (z * 4 + dev_q, head))

    def span(rb):
        return pl.ds(pl.multiple_of((rb % 2) * H, H), H)

    def project(rb, yd, half):
        r = (((y + yd) % 4) * 2 + half + NZ - z) % NZ
        total = None
        for pr in range(PAIRS):
            part = dot(a_all[rb // 2, pr, span(rb), :], w_all[r, pr * C:(pr + 1) * C, :])
            total = part if total is None else total + part
        return total

    def first_stage(rb):
        for way in range(2):
            tx[rb, way, 0] = project(rb, 2, way).astype(BF16)
            start(ycopy(rb, way, 0))
        for way in range(2):
            tx[rb, way, 1] = project(rb, 1 if way == 0 else 3, 1 - way).astype(BF16)
            start(ycopy(rb, way, 1))
        for way in range(2):
            keep[rb, way] = project(rb, 1 if way == 0 else 3, way)
        for half in range(2):
            keep[rb, 2 + half] = project(rb, 0, half)

    def second_stage(rb):
        for way in range(2):
            got(ycopy(rb, way, 0))
            tx[rb, way, 2] = (keep[rb, way] + rx[rb, way, 0].astype(F32)).astype(BF16)
            start(ycopy(rb, way, 2))

    def third_stage(rb):
        for n in (1, 2):
            for way in range(2):
                got(ycopy(rb, way, n))
        for half in range(2):
            keep[rb, 2 + half] = keep[rb, 2 + half] + (
                rx[rb, half, 2].astype(F32) + rx[rb, 1 - half, 1].astype(F32))
        xtx[rb] = keep[rb, 3 - xh].astype(BF16)
        start(hcopy(rb))

    def fourth_stage(rb):
        got(hcopy(rb))
        total = (keep[rb, 2 + xh] + xrx[rb].astype(F32)).astype(BF16)
        fin[rb] = total

        @pl.when(rb // 2 != q)
        def _():
            start(ocopy(rb, rb // 2, q))

    def rb_loop(t, carry):
        for lag, (stage) in enumerate((first_stage, second_stage, third_stage, fourth_stage)):
            @pl.when((t >= lag) & (t < 8 + lag))
            def _():
                stage(t - lag)
        return carry

    lax.fori_loop(0, 11, rb_loop, 0)
    for n in range(2):
        out_ref[n * H:(n + 1) * H, pl.ds(pl.multiple_of(q * C, C), C)] = fin[2 * q + n]

    for i in range(2):
        for dz in range(3):
            kv_z(dz, i).wait_send()
        for dz in range(4):
            only(dz, low, high, lambda: kv_x(dz, i).wait_send())
            only(dz, even, odd, lambda: kv_s(dz, i).wait_send())
            only(dz, high, low, lambda: kv_f(dz, i).wait_send())
    for hf in range(4):
        for n in range(4):
            w_dn(n, hf).wait_send()
        for n in range(3):
            w_up(n, hf).wait_send()
    for pr in range(PAIRS):
        for c in (a_x(pr), a_s(pr), a_f(pr)):
            c.wait_send()

    def finish(rb, carry):
        for way in range(2):
            for n in range(3):
                ycopy(rb, way, n).wait_send()
        hcopy(rb).wait_send()

        @pl.when(rb // 2 != q)
        def _():
            ocopy(rb, rb // 2, q).wait_send()
            ocopy(rb, rb // 2, rb // 2).wait_recv()

        return carry

    lax.fori_loop(0, 8, finish, 0)


def body(queries, keys, values, windows, out_weight):
    dma = pltpu.SemaphoreType.DMA
    vm = pl.BlockSpec(memory_space=pltpu.VMEM)
    hbm = pl.BlockSpec(memory_space=pl.ANY)
    return pl.pallas_call(
        kernel,
        out_shape=jax.ShapeDtypeStruct((T, 4 * C), BF16),
        in_specs=[vm, hbm, vm, pl.BlockSpec(memory_space=pltpu.SMEM), hbm],
        out_specs=vm,
        scratch_shapes=[
            pltpu.VMEM((PAIRS, ROWS, DH), BF16),
            pltpu.VMEM((19, T, DH), BF16),
            pltpu.VMEM((19, VR, T), BF16),
            pltpu.VMEM((NZ, QPG * DH, C), BF16),
            pltpu.VMEM((4, PAIRS, T, C), BF16),
            pltpu.VMEM((4, T, ROWS), F32),
            pltpu.VMEM((PAIRS, 1, ROWS), F32),
            pltpu.VMEM((PAIRS, VR, ROWS), F32),
            pltpu.VMEM((36, 1, ROWS), F32),
            pltpu.VMEM((T, T), F32),
            pltpu.VMEM((3, 128, DH), BF16),
            pltpu.VMEM((3, VR, 128), BF16),
            pltpu.VMEM((3, 128, 128), F32),
            pltpu.VMEM((8, 2, 3, H, C), BF16),
            pltpu.VMEM((8, 2, 3, H, C), BF16),
            pltpu.VMEM((8, 4, H, C), F32),
            pltpu.VMEM((8, H, C), BF16),
            pltpu.VMEM((8, H, C), BF16),
            pltpu.VMEM((8, H, C), BF16),
            dma((2,)),
            dma((3, 2)), dma((3, 2)),
            dma((4, 2)), dma((4, 2)),
            dma((4, 2)), dma((4, 2)),
            dma((4, 2)), dma((4, 2)),
            dma((4, 4)), dma((4, 4)),
            dma((3, 4)), dma((3, 4)),
            dma((PAIRS,)), dma((PAIRS,)),
            dma((PAIRS,)), dma((PAIRS,)),
            dma((PAIRS,)), dma((PAIRS,)),
            dma((8, 2, 3)), dma((8, 2, 3)),
            dma((8,)), dma((8,)),
            dma((8,)), dma((4, 2)),
        ],
        compiler_params=pltpu.CompilerParams(
            collective_id=0, has_side_effects=True, vmem_limit_bytes=60 * 1024 * 1024),
        name="fused",
    )(queries, keys, values, windows, out_weight)


def solution(mesh):
    placed = (P("seq", "head"), P("seq", "head"), P("seq", "head"), P("head"), P("head", "seq"))
    return jax.shard_map(
        body, mesh=mesh, in_specs=placed, out_specs=P("seq", "head"), check_vma=False
    )
```

```python
import math

import jax
import jax.numpy as jnp
from jax import lax
from jax.experimental import pallas as pl
from jax.experimental.pallas import tpu as pltpu
from jax.sharding import PartitionSpec as P

MESH = pl.DeviceIdType.MESH
DH = 128
QPG = 8
T = 384
NZ = 8
H = T // 2
NEG = -1e30
ROWS = 2 * T
PAIRS = QPG // 2
VR = DH + 16
C = 256
F32 = jnp.float32
BF16 = jnp.bfloat16
NT = (((1,), (1,)), ((), ()))
NN = (((1,), (0,)), ((), ()))


def dot(a, b, dims=NN):
    return lax.dot_general(a, b, dims, preferred_element_type=F32)


def kernel(q_ref, k_ref, v_ref, win_ref, w_ref, out_ref,
           qs, k_all, vt_all, w_all, a_all, s_ref, m_ref, acc_ref, fb_ref, bias0, kb, vb, tb,
           tx, rx, keep, xtx, xrx, fin,
           lsem, zs, zr, xs, xr, ss, sr, fs, fr, wds, wdr, wus, wur,
           axs, axr, ass, asr, afs, afr, ys, yr, hs, hr, os, orr):
    seq = lax.axis_index("seq")
    head = lax.axis_index("head")
    z = seq // 4
    q = seq % 4
    y = head // 2
    xh = head % 2
    q1 = q + 1 - 2 * (q % 2)
    q2 = (q + 2) % 4
    q3 = q1 + 2 - 4 * (q1 // 2)
    zup = (((z + 1) % NZ) * 4 + q, head)
    zdn = (((z + NZ - 1) % NZ) * 4 + q, head)
    sib = (z * 4 + q1, head)
    xlo = (z * 4 + q2, head)
    dia = (z * 4 + q3, head)
    yup = (seq, ((y + 1) % 4) * 2 + xh)
    ydn = (seq, ((y + 3) % 4) * 2 + xh)
    xhi = (seq, y * 2 + 1 - xh)

    def rc(src, dst, ssem, rsem, dev):
        return pltpu.make_async_remote_copy(
            src_ref=src, dst_ref=dst, send_sem=ssem, recv_sem=rsem, device_id=dev, device_id_type=MESH)

    lk = pltpu.make_async_copy(k_ref, k_all.at[3], lsem.at[0])
    lw = pltpu.make_async_copy(w_ref, w_all.at[0], lsem.at[1])
    lk.start()
    lw.start()
    barrier = pltpu.get_barrier_semaphore()
    for dev in (zup, zdn, sib, xlo, dia, yup, ydn, xhi):
        pl.semaphore_signal(barrier, inc=1, device_id=dev, device_id_type=MESH)
    for slot in range(19):
        vt_all[slot, DH:VR, :] = jnp.ones((VR - DH, T), BF16)
    vt_all[3, 0:DH, :] = v_ref[...].astype(F32).T.astype(BF16)
    lk.wait()
    lw.wait()
    pl.semaphore_wait(barrier, 8)

    def kv(src_slot, dst_slot, ssem, rsem, n, i, dev):
        if i == 0:
            return rc(k_all.at[src_slot], k_all.at[dst_slot], ssem.at[n, 0], rsem.at[n, 0], dev)
        return rc(vt_all.at[src_slot, pl.ds(0, DH)], vt_all.at[dst_slot, pl.ds(0, DH)],
                  ssem.at[n, 1], rsem.at[n, 1], dev)

    def kv_z(dz, i):
        return kv(3 + 4 * dz, 7 + 4 * dz, zs, zr, dz, i, zup)

    def kv_x(dz, i):
        return kv(3 + 4 * dz, 3 + 4 * dz + q2 - q, xs, xr, dz, i, xlo)

    def kv_s(dz, i):
        return kv(3 + 4 * dz, 3 + 4 * dz + q1 - q, ss, sr, dz, i, sib)

    def kv_f(dz, i):
        return kv(3 + 4 * dz + q - q2, 3 + 4 * dz + q1 - q2, fs, fr, dz, i, sib)

    def only(dz, near, far, act):
        if dz in (1, 2):
            act()
        else:
            pl.when(near if dz == 0 else far)(act)

    low, even = q < 2, q % 2 == 0
    high, odd = q >= 2, q % 2 == 1

    def send_z(dz, i):
        kv_z(dz, i).start()

    def send_xs(dz, i):
        only(dz, low, high, lambda: kv_x(dz, i).start())
        only(dz, even, odd, lambda: kv_s(dz, i).start())

    def pass_f(dz, i):
        def act():
            kv_x(dz, i).wait_recv()
            kv_f(dz, i).start()
        only(dz, high, low, act)

    def got_sf(dz):
        for i in range(2):
            only(dz, odd, even, lambda: kv_s(dz, i).wait_recv())
            only(dz, high, low, lambda: kv_f(dz, i).wait_recv())

    def w_dn(n, hf):
        rows = pl.ds(hf * 256, 256)
        return rc(w_all.at[n, rows], w_all.at[n + 1, rows], wds.at[n, hf], wdr.at[n, hf], zdn)

    def w_up(n, hf):
        rows = pl.ds(hf * 256, 256)
        return rc(w_all.at[(NZ - n) % NZ, rows], w_all.at[NZ - 1 - n, rows], wus.at[n, hf], wur.at[n, hf], zup)

    def start(*copies):
        for c in copies:
            c.start()

    def got(*copies):
        for c in copies:
            c.wait_recv()

    def pass_dn(n, hf):
        got(w_dn(n, hf))
        start(w_dn(n + 1, hf))

    def pass_up(n, hf):
        got(w_up(n, hf))
        start(w_up(n + 1, hf))

    for i in range(2):
        send_z(0, i)
        send_xs(0, i)
    start(*[w_dn(0, hf) for hf in range(4)], w_up(0, 0))

    for p in range(QPG):
        qs[p // 2, (p % 2) * T:(p % 2 + 1) * T, :] = (
            q_ref[:, p * DH:(p + 1) * DH].astype(F32) * (math.log2(math.e) / math.sqrt(DH))).astype(BF16)
    wn = win_ref[0] // 128
    col = lax.broadcasted_iota(jnp.int32, (1, ROWS), 1)
    ctile = sum(jnp.where(col >= 128 * n, 1, 0) for n in range(1, 6))
    iq = ctile - 3 * jnp.where(ctile >= 3, 1, 0)
    for d in range(1, 12):
        for jk in range(3):
            inside = (3 * d - jk + iq < wn) & (seq - d >= 0)
            fb_ref[d * 3 + jk] = jnp.where(inside, 0.0, NEG)
    kj = lax.broadcasted_iota(jnp.int32, (T, T), 0)
    qi = lax.broadcasted_iota(jnp.int32, (T, T), 1)
    kt = jnp.where(kj >= 128, 1, 0) + jnp.where(kj >= 256, 1, 0)
    qt = jnp.where(qi >= 128, 1, 0) + jnp.where(qi >= 256, 1, 0)
    bias0[...] = jnp.where((kj <= qi) & (qt - kt < wn), 0.0, NEG)

    def group(dlist, first, last, service=()):
        def pair_body(pr, carry):
            for at, act in service:
                pl.when(pr == at)(act)
            qp = qs[pr]
            mx = None
            for b, d in enumerate(dlist):
                s = dot(k_all[d + 3], qp, NT)
                if d == 0:
                    s = s + jnp.concatenate([bias0[...], bias0[...]], axis=1)
                s_ref[b] = s
                for jk in range(3):
                    t8 = jnp.max(s[jk * 128:(jk + 1) * 128].reshape(16, 8, ROWS), axis=0)
                    if d > 0:
                        t8 = t8 + fb_ref[d * 3 + jk]
                    mx = t8 if mx is None else jnp.maximum(mx, t8)
            edge = []
            if last:
                for c in range(6):
                    sb = dot(kb[c % 3], qp[c * 128:(c + 1) * 128], NT) + tb[c % 3]
                    edge.append(sb)
                e8 = [jnp.max(sb.reshape(16, 8, 128), axis=0) for sb in edge]
                mx = jnp.maximum(mx, jnp.concatenate(e8, axis=1))
            m_new = jnp.max(mx, axis=0, keepdims=True)
            if not first:
                m_old = m_ref[pr]
                m_new = jnp.maximum(m_old, m_new)
                alpha = jnp.exp2(m_old - m_new)
            pv = None
            for b, d in enumerate(dlist):
                tiles = []
                for jk in range(3):
                    shift = m_new - fb_ref[d * 3 + jk] if d > 0 else m_new
                    tiles.append(jnp.exp2(s_ref[b, jk * 128:(jk + 1) * 128, :] - shift).astype(BF16))
                part = dot(vt_all[d + 3], jnp.concatenate(tiles, axis=0))
                pv = part if pv is None else pv + part
            if last:
                ep = []
                for c in range(6):
                    pe = jnp.exp2(edge[c] - m_new[:, c * 128:(c + 1) * 128]).astype(BF16)
                    ep.append(dot(vb[c % 3], pe))
                pv = pv + jnp.concatenate(ep, axis=1)
            if not first:
                pv = acc_ref[pr] * alpha + pv
            if last:
                o = pv[0:DH] / pv[DH:DH + 1]
                for h in range(2):
                    a_all[q, pr, :, h * DH:(h + 1) * DH] = o[:, h * T:(h + 1) * T].T.astype(BF16)
                start(a_x(pr), a_s(pr))
            else:
                acc_ref[pr] = pv
                m_ref[pr] = m_new
            return carry

        lax.fori_loop(0, PAIRS, pair_body, 0)

    def a_x(pr):
        return rc(a_all.at[q, pr], a_all.at[q, pr], axs.at[pr], axr.at[pr], xlo)

    def a_s(pr):
        return rc(a_all.at[q, pr], a_all.at[q, pr], ass.at[pr], asr.at[pr], sib)

    def a_f(pr):
        return rc(a_all.at[q2, pr], a_all.at[q2, pr], afs.at[pr], afr.at[pr], sib)

    group((0,), True, False)
    for i in range(2):
        got(kv_z(0, i))
        send_z(1, i)
        send_xs(1, i)
    start(w_up(0, 1))
    for i in range(2):
        pass_f(0, i)
    for i in range(2):
        got(kv_z(1, i))
        send_z(2, i)
        send_xs(2, i)
    start(w_up(0, 2), w_up(0, 3))
    pass_dn(0, 0)
    pass_dn(0, 1)
    for i in range(2):
        pass_f(1, i)
    pass_dn(0, 2)
    got_sf(0)
    got_sf(1)

    def in_first():
        for i in range(2):
            got(kv_z(2, i))
            send_xs(3, i)
        pass_dn(0, 3)
        pass_up(0, 0)

    group((1, 2, 3), False, False, ((2, in_first),))
    for i in range(2):
        pass_f(2, i)
    pass_dn(1, 0)
    got_sf(2)

    def in_second():
        pass_dn(1, 1)
        pass_up(0, 1)
        for i in range(2):
            pass_f(3, i)

    def late_second():
        pass_dn(1, 2)
        pass_up(0, 2)

    group((4, 5, 6, 7), False, False, ((1, in_second), (3, late_second)))
    got_sf(3)
    pass_dn(1, 3)
    pass_up(0, 3)

    def in_third():
        pass_dn(2, 0)
        pass_up(1, 0)

    def late_third():
        pass_dn(2, 1)
        pass_up(1, 1)

    ej = lax.broadcasted_iota(jnp.int32, (128, 128), 0)
    ei = lax.broadcasted_iota(jnp.int32, (128, 128), 1)
    for n in range(3):
        kn = jnp.zeros((128, DH), BF16)
        vn = jnp.zeros((VR, 128), BF16)
        for d in range(12):
            for jk in range(3):
                if 2 <= 3 * d + n - jk <= 32:
                    here = wn == 3 * d + n - jk
                    kn = jnp.where(here, k_all[d + 3, jk * 128:(jk + 1) * 128, :], kn)
                    vn = jnp.where(here, vt_all[d + 3, :, jk * 128:(jk + 1) * 128], vn)
        kb[n] = kn
        vb[n] = vn
        tb[n] = jnp.where((ej > ei) & (3 * seq + n - wn >= 0), 0.0, NEG)
    group((8, 9, 10, 11), False, True, ((1, in_third), (3, late_third)))
    for hf in (2, 3):
        pass_dn(2, hf)
        pass_up(1, hf)
    for hf in range(4):
        got(w_dn(3, hf), w_up(2, hf))

    def ycopy(rb, way, n):
        return rc(tx.at[rb, way, n], rx.at[rb, way, n], ys.at[rb, way, n], yr.at[rb, way, n], yup if way == 0 else ydn)

    def hcopy(rb):
        return rc(xtx.at[rb], xrx.at[rb], hs.at[rb], hr.at[rb], xhi)

    def ocopy(rb, dev_q, slot):
        rows, cols = span(rb), pl.ds(pl.multiple_of(slot * C, C), C)
        return rc(fin.at[rb], out_ref.at[rows, cols], os.at[rb], orr.at[slot, rb % 2], (z * 4 + dev_q, head))

    def span(rb):
        return pl.ds(pl.multiple_of((rb % 2) * H, H), H)

    def project(rb, yd, half):
        r = (((y + yd) % 4) * 2 + half + NZ - z) % NZ
        total = None
        for pr in range(PAIRS):
            part = dot(a_all[rb // 2, pr, span(rb), :], w_all[r, pr * C:(pr + 1) * C, :])
            total = part if total is None else total + part
        return total

    def first_stage(rb):
        for way in range(2):
            tx[rb, way, 0] = project(rb, 2, way).astype(BF16)
            start(ycopy(rb, way, 0))
        for way in range(2):
            tx[rb, way, 1] = project(rb, 1 if way == 0 else 3, 1 - way).astype(BF16)
            start(ycopy(rb, way, 1))
        for way in range(2):
            keep[rb, way] = project(rb, 1 if way == 0 else 3, way)
        for half in range(2):
            keep[rb, 2 + half] = project(rb, 0, half)

    def second_stage(rb):
        for way in range(2):
            got(ycopy(rb, way, 0))
            tx[rb, way, 2] = (keep[rb, way] + rx[rb, way, 0].astype(F32)).astype(BF16)
            start(ycopy(rb, way, 2))

    def third_stage(rb):
        for n in (1, 2):
            for way in range(2):
                got(ycopy(rb, way, n))
        for half in range(2):
            keep[rb, 2 + half] = keep[rb, 2 + half] + (
                rx[rb, half, 2].astype(F32) + rx[rb, 1 - half, 1].astype(F32))
        xtx[rb] = keep[rb, 3 - xh].astype(BF16)
        start(hcopy(rb))

    def fourth_stage(rb):
        got(hcopy(rb))
        total = (keep[rb, 2 + xh] + xrx[rb].astype(F32)).astype(BF16)
        fin[rb] = total

        @pl.when(rb // 2 != q)
        def _():
            start(ocopy(rb, rb // 2, q))

    def chunk(t):
        n = t // 2
        return (((q // 2 + n // 2) % 2) * 2 + (q + n) % 2) * 2 + t % 2

    def rb_loop(t, carry):
        @pl.when(t == 1)
        def _():
            for pr in range(PAIRS):
                got(a_x(pr))
                start(a_f(pr))

        @pl.when(t == 2)
        def _():
            for pr in range(PAIRS):
                got(a_s(pr))

        @pl.when(t == 6)
        def _():
            for pr in range(PAIRS):
                got(a_f(pr))

        for lag, stage in enumerate((first_stage, second_stage, third_stage, fourth_stage)):
            @pl.when((t >= lag) & (t < 8 + lag))
            def _():
                stage(chunk(t - lag))
        return carry

    lax.fori_loop(0, 11, rb_loop, 0)
    for n in range(2):
        out_ref[n * H:(n + 1) * H, pl.ds(pl.multiple_of(q * C, C), C)] = fin[2 * q + n]

    for i in range(2):
        for dz in range(3):
            kv_z(dz, i).wait_send()
        for dz in range(4):
            only(dz, low, high, lambda: kv_x(dz, i).wait_send())
            only(dz, even, odd, lambda: kv_s(dz, i).wait_send())
            only(dz, high, low, lambda: kv_f(dz, i).wait_send())
    for hf in range(4):
        for n in range(4):
            w_dn(n, hf).wait_send()
        for n in range(3):
            w_up(n, hf).wait_send()
    for pr in range(PAIRS):
        for c in (a_x(pr), a_s(pr), a_f(pr)):
            c.wait_send()

    def finish(rb, carry):
        for way in range(2):
            for n in range(3):
                ycopy(rb, way, n).wait_send()
        hcopy(rb).wait_send()

        @pl.when(rb // 2 != q)
        def _():
            ocopy(rb, rb // 2, q).wait_send()
            ocopy(rb, rb // 2, rb // 2).wait_recv()

        return carry

    lax.fori_loop(0, 8, finish, 0)


def body(queries, keys, values, windows, out_weight):
    dma = pltpu.SemaphoreType.DMA
    vm = pl.BlockSpec(memory_space=pltpu.VMEM)
    hbm = pl.BlockSpec(memory_space=pl.ANY)
    return pl.pallas_call(
        kernel,
        out_shape=jax.ShapeDtypeStruct((T, 4 * C), BF16),
        in_specs=[vm, hbm, vm, pl.BlockSpec(memory_space=pltpu.SMEM), hbm],
        out_specs=vm,
        scratch_shapes=[
            pltpu.VMEM((PAIRS, ROWS, DH), BF16),
            pltpu.VMEM((19, T, DH), BF16),
            pltpu.VMEM((19, VR, T), BF16),
            pltpu.VMEM((NZ, QPG * DH, C), BF16),
            pltpu.VMEM((4, PAIRS, T, C), BF16),
            pltpu.VMEM((4, T, ROWS), F32),
            pltpu.VMEM((PAIRS, 1, ROWS), F32),
            pltpu.VMEM((PAIRS, VR, ROWS), F32),
            pltpu.VMEM((36, 1, ROWS), F32),
            pltpu.VMEM((T, T), F32),
            pltpu.VMEM((3, 128, DH), BF16),
            pltpu.VMEM((3, VR, 128), BF16),
            pltpu.VMEM((3, 128, 128), F32),
            pltpu.VMEM((8, 2, 3, H, C), BF16),
            pltpu.VMEM((8, 2, 3, H, C), BF16),
            pltpu.VMEM((8, 4, H, C), F32),
            pltpu.VMEM((8, H, C), BF16),
            pltpu.VMEM((8, H, C), BF16),
            pltpu.VMEM((8, H, C), BF16),
            dma((2,)),
            dma((3, 2)), dma((3, 2)),
            dma((4, 2)), dma((4, 2)),
            dma((4, 2)), dma((4, 2)),
            dma((4, 2)), dma((4, 2)),
            dma((4, 4)), dma((4, 4)),
            dma((3, 4)), dma((3, 4)),
            dma((PAIRS,)), dma((PAIRS,)),
            dma((PAIRS,)), dma((PAIRS,)),
            dma((PAIRS,)), dma((PAIRS,)),
            dma((8, 2, 3)), dma((8, 2, 3)),
            dma((8,)), dma((8,)),
            dma((8,)), dma((4, 2)),
        ],
        compiler_params=pltpu.CompilerParams(
            collective_id=0, has_side_effects=True, vmem_limit_bytes=60 * 1024 * 1024),
        name="fused",
    )(queries, keys, values, windows, out_weight)


def solution(mesh):
    placed = (P("seq", "head"), P("seq", "head"), P("seq", "head"), P("head"), P("head", "seq"))
    return jax.shard_map(
        body, mesh=mesh, in_specs=placed, out_specs=P("seq", "head"), check_vma=False
    )
```
